128 devices in a mesh: pod: 1, dp: 64 (over z, y, x), tp: 2 (over core).
Axes of the slice: x: 4, y: 4, z: 4, core: 2. Of those that a mesh axis runs over, the one named last changes fastest.
Arguments:
- tokens: bfloat16 [128, 256, 2048], P(('pod', 'dp'))
- seg_ids: int32 [128, 256], P(('pod', 'dp'))
- grad_out: bfloat16 [128, 256, 2048], P(('pod', 'dp'))
- gain_attn: float32 [2048], replicated
- gain_mlp: float32 [2048], replicated
- w_query: bfloat16 [2048, 2048], P(None, 'tp')
- w_key: bfloat16 [2048, 1024], P(None, 'tp')
- w_value: bfloat16 [2048, 1024], P(None, 'tp')
- w_out: bfloat16 [2048, 2048], P('tp')
- w_gate: bfloat16 [2048, 6144], P(None, 'tp')
- w_up: bfloat16 [2048, 6144], P(None, 'tp')
- w_down: bfloat16 [6144, 2048], P('tp')
Outputs:
- output 1: bfloat16 [128, 256, 2048], P(('pod', 'dp'))
- output 2: bfloat16 [128, 256, 2048], P(('pod', 'dp'))
- output 3: float32 [2048], P('pod')
- output 4: float32 [2048], P('pod')
- output 5: float32 [2048, 2048], P(('pod', 'dp'), 'tp')
- output 6: float32 [2048, 1024], P(('pod', 'dp'), 'tp')
- output 7: float32 [2048, 1024], P(('pod', 'dp'), 'tp')
- output 8: float32 [2048, 2048], P(('pod', 'tp', 'dp'))
- output 9: float32 [2048, 6144], P(('pod', 'dp'), 'tp')
- output 10: float32 [2048, 6144], P(('pod', 'dp'), 'tp')
- output 11: float32 [6144, 2048], P(('pod', 'tp', 'dp'))
All inputs are finite; a program needn't handle non-finite values.
Results may differ from the reference program's by a relative error of at most 0.02.
Values are sent between devices in bfloat16 or wider.
A program may use at most 1 GiB of HBM per device.

```python
import functools
import jax
import jax.numpy as jnp
from jax import lax

MODEL_DIM = 2048
FFN_DIM = 6144
Q_HEADS = 16
KV_HEADS = 8
HEAD_DIM = 128
SEQ_LEN = 256
BATCH_ROWS = 128


def draw_segments(seg_key):
    count_key, cut_key = jax.random.split(seg_key)
    cuts_per_row = jax.random.randint(count_key, (BATCH_ROWS, 1), 0, 8)
    cut_draw = jax.random.randint(cut_key, (BATCH_ROWS, SEQ_LEN), 0, SEQ_LEN)
    positions = jnp.arange(SEQ_LEN)[None, :]
    starts = jnp.where((cut_draw < cuts_per_row) & (positions > 0), 1, 0)
    return jnp.cumsum(starts, axis=1).astype(jnp.int32)


def normal_weight(weight_key, shape, scale):
    return (jax.random.normal(weight_key, shape, jnp.float32) * scale).astype(jnp.bfloat16)


def setup_inputs(seed: int = 0, part: int = 0) -> dict:
    base_key = jax.random.key(seed)
    part_keys = jax.random.split(jax.random.fold_in(base_key, part), 3)
    shared_keys = jax.random.split(base_key, 9)
    row_shape = (BATCH_ROWS, SEQ_LEN, MODEL_DIM)
    q_width = Q_HEADS * HEAD_DIM
    kv_width = KV_HEADS * HEAD_DIM
    return {
        "tokens": normal_weight(part_keys[0], row_shape, 1.0),
        "seg_ids": draw_segments(part_keys[2]),
        "grad_out": normal_weight(part_keys[1], row_shape, 1.0),
        "gain_attn": jax.random.uniform(shared_keys[0], (MODEL_DIM,), jnp.float32, 0.5, 1.5),
        "gain_mlp": jax.random.uniform(shared_keys[1], (MODEL_DIM,), jnp.float32, 0.5, 1.5),
        "w_query": normal_weight(shared_keys[2], (MODEL_DIM, q_width), (2.0 / MODEL_DIM) ** 0.5),
        "w_key": normal_weight(shared_keys[3], (MODEL_DIM, kv_width), (2.0 / MODEL_DIM) ** 0.5),
        "w_value": normal_weight(shared_keys[4], (MODEL_DIM, kv_width), MODEL_DIM ** -0.5),
        "w_out": normal_weight(shared_keys[5], (q_width, MODEL_DIM), 2.0 * q_width ** -0.5),
        "w_gate": normal_weight(shared_keys[6], (MODEL_DIM, FFN_DIM), MODEL_DIM ** -0.5),
        "w_up": normal_weight(shared_keys[7], (MODEL_DIM, FFN_DIM), MODEL_DIM ** -0.5),
        "w_down": normal_weight(shared_keys[8], (FFN_DIM, MODEL_DIM), 2.0 * FFN_DIM ** -0.5),
    }


def rms_scale(values, gain):
    mean_square = jnp.mean(values * values, axis=-1, keepdims=True)
    return values * lax.rsqrt(mean_square + 1e-5) * gain


def gate_mix(gate_pre, up_pre):
    return (jax.nn.silu(gate_pre.astype(jnp.float32)) * up_pre.astype(jnp.float32)).astype(jnp.bfloat16)


def attend_one(query_grp, key_one, value_one, seg_row):
    scores = jnp.einsum("qgd,sd->gqs", query_grp.astype(jnp.float32), key_one.astype(jnp.float32)) * (HEAD_DIM ** -0.5)
    positions = jnp.arange(SEQ_LEN)
    allowed = (positions[None, :] <= positions[:, None]) & (seg_row[None, :] == seg_row[:, None])
    scores = jnp.where(allowed[None], scores, -1e30)
    attn_probs = jax.nn.softmax(scores, axis=-1).astype(jnp.bfloat16)
    context = jnp.einsum("gqs,sd->qgd", attn_probs.astype(jnp.float32), value_one.astype(jnp.float32))
    return context.astype(jnp.bfloat16)


def head_forward(bundle):
    return attend_one(bundle[0], bundle[1], bundle[2], bundle[3])


def head_backward(bundle):
    attn_vjp = jax.vjp(functools.partial(attend_one, seg_row=bundle[3]), bundle[0], bundle[1], bundle[2])[1]
    return attn_vjp(bundle[4])


def to_heads(flat, per_kv):
    n_rows = flat.shape[0] // SEQ_LEN
    split = flat.reshape(n_rows, SEQ_LEN, KV_HEADS, per_kv, HEAD_DIM)
    return split.transpose(0, 2, 1, 3, 4).reshape(n_rows * KV_HEADS, SEQ_LEN, per_kv, HEAD_DIM)


def from_heads(heads):
    n_rows = heads.shape[0] // KV_HEADS
    split = heads.reshape(n_rows, KV_HEADS, SEQ_LEN, -1, HEAD_DIM)
    return split.transpose(0, 2, 1, 3, 4).reshape(n_rows * SEQ_LEN, -1)


def reference(tokens, seg_ids, grad_out, gain_attn, gain_mlp, w_query, w_key, w_value, w_out, w_gate, w_up, w_down):
    n_rows = tokens.shape[0]
    n_tokens = n_rows * SEQ_LEN
    group_size = Q_HEADS // KV_HEADS
    x_float = tokens.reshape(n_tokens, MODEL_DIM).astype(jnp.float32)
    norm_attn, attn_norm_vjp = jax.vjp(rms_scale, x_float, gain_attn)
    attn_in = norm_attn.astype(jnp.bfloat16)
    query = jnp.dot(attn_in, w_query, preferred_element_type=jnp.float32).astype(jnp.bfloat16)
    key_proj = jnp.dot(attn_in, w_key, preferred_element_type=jnp.float32).astype(jnp.bfloat16)
    value_proj = jnp.dot(attn_in, w_value, preferred_element_type=jnp.float32).astype(jnp.bfloat16)
    head_inputs = (to_heads(query, group_size), to_heads(key_proj, 1)[:, :, 0, :], to_heads(value_proj, 1)[:, :, 0, :], jnp.repeat(seg_ids, KV_HEADS, axis=0))
    context = from_heads(lax.map(head_forward, head_inputs))
    attn_sum = jnp.dot(context, w_out, preferred_element_type=jnp.float32).astype(jnp.bfloat16)
    hidden_float = (x_float + attn_sum.astype(jnp.float32)).astype(jnp.bfloat16).astype(jnp.float32)
    norm_mlp, mlp_norm_vjp = jax.vjp(rms_scale, hidden_float, gain_mlp)
    mlp_in = norm_mlp.astype(jnp.bfloat16)
    gate_pre = jnp.dot(mlp_in, w_gate, preferred_element_type=jnp.float32).astype(jnp.bfloat16)
    up_pre = jnp.dot(mlp_in, w_up, preferred_element_type=jnp.float32).astype(jnp.bfloat16)
    mixed_act, mix_vjp = jax.vjp(gate_mix, gate_pre, up_pre)
    mlp_sum = jnp.dot(mixed_act, w_down, preferred_element_type=jnp.float32).astype(jnp.bfloat16)
    layer_out = (hidden_float + mlp_sum.astype(jnp.float32)).astype(jnp.bfloat16)
    grad_flat = grad_out.reshape(n_tokens, MODEL_DIM)
    d_mixed = jnp.dot(grad_flat, w_down.T, preferred_element_type=jnp.float32).astype(jnp.bfloat16)
    d_gate, d_up = mix_vjp(d_mixed)
    d_mlp_in = (jnp.dot(d_gate, w_gate.T, preferred_element_type=jnp.float32) + jnp.dot(d_up, w_up.T, preferred_element_type=jnp.float32)).astype(jnp.bfloat16)
    d_hidden_part, grad_gain_mlp = mlp_norm_vjp(d_mlp_in.astype(jnp.float32))
    d_hidden = grad_flat.astype(jnp.float32) + d_hidden_part
    d_hidden_b = d_hidden.astype(jnp.bfloat16)
    d_context = jnp.dot(d_hidden_b, w_out.T, preferred_element_type=jnp.float32).astype(jnp.bfloat16)
    d_query_h, d_key_h, d_value_h = lax.map(head_backward, head_inputs + (to_heads(d_context, group_size),))
    d_query = from_heads(d_query_h)
    d_key = from_heads(d_key_h[:, :, None, :])
    d_value = from_heads(d_value_h[:, :, None, :])
    d_attn_in = (jnp.dot(d_query, w_query.T, preferred_element_type=jnp.float32) + jnp.dot(d_key, w_key.T, preferred_element_type=jnp.float32) + jnp.dot(d_value, w_value.T, preferred_element_type=jnp.float32)).astype(jnp.bfloat16)
    d_tokens_part, grad_gain_attn = attn_norm_vjp(d_attn_in.astype(jnp.float32))
    grad_tokens = (d_hidden + d_tokens_part).astype(jnp.bfloat16).reshape(n_rows, SEQ_LEN, MODEL_DIM)
    return (
        layer_out.reshape(n_rows, SEQ_LEN, MODEL_DIM),
        grad_tokens,
        grad_gain_attn,
        grad_gain_mlp,
        jnp.dot(attn_in.T, d_query, preferred_element_type=jnp.float32),
        jnp.dot(attn_in.T, d_key, preferred_element_type=jnp.float32),
        jnp.dot(attn_in.T, d_value, preferred_element_type=jnp.float32),
        jnp.dot(context.T, d_hidden_b, preferred_element_type=jnp.float32),
        jnp.dot(mlp_in.T, d_gate, preferred_element_type=jnp.float32),
        jnp.dot(mlp_in.T, d_up, preferred_element_type=jnp.float32),
        jnp.dot(mixed_act.T, grad_flat, preferred_element_type=jnp.float32),
    )
```

```python
import functools
import jax
import jax.numpy as jnp
from jax import lax
from jax.experimental import pallas as pl
from jax.experimental.pallas import tpu as pltpu
from jax.sharding import PartitionSpec as P

HEAD_DIM = 128
NORM_EPS = 1e-5
STEPS = (1, 3, 2)
STRIDE = {"z": 16, "y": 4, "x": 1}


def chip_coords():
    chip = lax.axis_index("dp")
    return {"z": chip // 16, "y": (chip // 4) % 4, "x": chip % 4}


def to_chip(chip, **coord):
    parts = {"z": chip // 16, "y": (chip // 4) % 4, "x": chip % 4}
    parts.update(coord)
    return 16 * (parts["z"] % 4) + 4 * (parts["y"] % 4) + parts["x"] % 4


def coord_of(chip, axis):
    return (chip // STRIDE[axis]) % 4


def shift(values, axis, step):
    pairs = [(c, to_chip(c, **{axis: coord_of(c, axis) + step})) for c in range(64)]
    return lax.ppermute(values, "dp", pairs)


def swap_cores(values):
    return lax.ppermute(values, "tp", [(0, 1), (1, 0)])


def sum_cores(part):
    other = swap_cores(part)
    return lax.reduce_precision(part.astype(jnp.float32) + other.astype(jnp.float32), 8, 7)


def pick(values, index, dim):
    return lax.dynamic_index_in_dim(values, index % values.shape[dim], dim, keepdims=False)


def gather_tokens(values, axis):
    return [values] + [shift(values, axis, d) for d in STEPS]


def gather_tokens_shared(values, axis):
    half = values.shape[0] // 2
    core = lax.axis_index("tp")
    row = lax.dynamic_slice_in_dim(values, core * half, half, 0)
    direct = [shift(row, axis, d) for d in STEPS]
    return [values] + direct + [swap_cores(v) for v in direct]


def exchange_columns(values, axis, at):
    width = values.shape[1] // 4
    return [shift(lax.dynamic_slice_in_dim(values, ((at[axis] + d) % 4) * width, width, 1), axis, d) for d in STEPS]


def add_parts(parts):
    return parts[0] + parts[1] + parts[2] + parts[3]


def scatter_parts(parts, axis):
    return add_parts([parts[0]] + [shift(parts[d], axis, d) for d in STEPS])


def exchange_kernel(routes, *refs):
    n = len(routes)
    sources, targets, (send_sem, recv_sem) = refs[:n], refs[n:2 * n], refs[2 * n:]
    chip = lax.axis_index("dp")
    barrier = pltpu.get_barrier_semaphore()
    for axis in "xyz":
        for d in STEPS:
            peer = to_chip(chip, **{axis: coord_of(chip, axis) + d})
            pl.semaphore_signal(barrier, inc=1, device_id={"dp": peer}, device_id_type=pl.DeviceIdType.MESH)
    pl.semaphore_wait(barrier, 9)
    copies = []
    for k, (axis, d) in enumerate(routes):
        peer = to_chip(chip, **{axis: coord_of(chip, axis) + d})
        copies.append(pltpu.make_async_remote_copy(
            src_ref=sources[k], dst_ref=targets[k], send_sem=send_sem.at[k], recv_sem=recv_sem.at[k],
            device_id={"dp": peer}, device_id_type=pl.DeviceIdType.MESH))
    for copy in copies:
        copy.start()
    for copy in copies:
        copy.wait()


def exchange(groups, call_id):
    routes, values = [], []
    for k in (1, 0, 2):
        for axis, parts in groups:
            routes.append((axis, k + 1))
            values.append(parts[k])
    any_spec = pl.BlockSpec(memory_space=pl.ANY)
    n = len(values)
    sent = sum(v.size * v.dtype.itemsize for v in values)
    out = pl.pallas_call(
        functools.partial(exchange_kernel, routes),
        in_specs=[any_spec] * n,
        out_specs=[any_spec] * n,
        out_shape=[jax.ShapeDtypeStruct(v.shape, v.dtype) for v in values],
        scratch_shapes=[pltpu.SemaphoreType.DMA((n,)), pltpu.SemaphoreType.DMA((n,))],
        compiler_params=pltpu.CompilerParams(collective_id=call_id, has_side_effects=True),
        cost_estimate=pl.CostEstimate(flops=0, bytes_accessed=2 * sent, transcendentals=0),
    )(*values)
    m = len(groups)
    by_step = dict(zip((1, 0, 2), (out[:m], out[m:2 * m], out[2 * m:])))
    return [[by_step[k][g] for k in range(3)] for g in range(m)]


def in_source_order(own, received, here):
    stacked = jnp.stack([own] + received)
    return [pick(stacked, here - b, 0) for b in range(4)]


def load_plan(own_rows, shared):
    half = own_rows // 2
    if not shared:
        return [(k, "all", own_rows, own_rows * k) for k in range(4)]
    plan = [(0, "all", own_rows, 0)]
    for group, which in enumerate(("mine", "other")):
        for k in range(3):
            plan.append((k + 1, which, half, own_rows + half * (3 * group + k)))
    return plan


def row_start(which, half, core):
    if which == "all":
        return 0
    return pl.multiple_of((core if which == "mine" else 1 - core) * half, half)


def dot_tokens(left, right):
    return lax.dot_general(left, right, (((0,), (0,)), ((), ())), preferred_element_type=jnp.float32)


def column_kernel(shared, split_right, width, n_chunks, info, *refs):
    n_left = 7 if shared else 4
    lefts, refs = refs[:n_left], refs[n_left:]
    n_right = 4 if split_right else 8
    rights, refs = refs[:n_right], refs[n_right:]
    hi_out, lo_out, refs = refs[:4], refs[4:8], refs[8:]
    left_buf, right_buf, acc, left_sem, right_sem, hi_sem, lo_sem = refs
    hi_at, lo_at, block, core = info[0], info[1], info[2], info[3]
    n_own = lefts[0].shape[0]
    half = n_own // 2
    plan = load_plan(n_own, shared)

    right_copies = []
    for side in range(2):
        for k, (source, which, rows, first) in enumerate(plan):
            ref = rights[source] if split_right else rights[4 * side + source]
            col = side * width if split_right else 0
            if source == 0 and not split_right:
                col = pl.multiple_of(block * width, 128)
            right_copies.append(pltpu.make_async_copy(
                ref.at[pl.ds(row_start(which, half, core), rows), pl.ds(col, width)],
                right_buf.at[pl.ds(first, rows), pl.ds(side * width, width)],
                right_sem.at[side, k]))
    for copy in right_copies:
        copy.start()

    def row_block(step):
        return lax.rem(hi_at + step + 1, 4)

    def left_copies(step, slot):
        col = pl.multiple_of(row_block(step) * 512, 512)
        for k, (source, which, rows, first) in enumerate(plan):
            ref = lefts[k] if shared else lefts[source]
            yield pltpu.make_async_copy(
                ref.at[:, pl.ds(col, 512)], left_buf.at[slot, pl.ds(first, rows), :], left_sem.at[slot, k])

    for copy in left_copies(0, 0):
        copy.start()
    for copy in right_copies:
        copy.wait()

    def lo_copies(step):
        rows = 128 // n_chunks
        for d in range(4):
            for k in range(n_chunks):
                first = pl.multiple_of(k * 128 + lax.rem(lo_at + d, 4) * rows, rows)
                yield pltpu.make_async_copy(
                    acc.at[step, pl.ds(first, rows), pl.ds(width, width)],
                    lo_out[d].at[row_block(step), pl.ds(k * rows, rows), :], lo_sem.at[step, d, k])

    def hi_copy(step, d):
        return pltpu.make_async_copy(acc.at[step, :, pl.ds(0, width)], hi_out[d], hi_sem.at[step])

    tile = 512 if (2 * width) % 512 == 0 else 256

    @pl.loop(0, 4)
    def _(step):
        slot = lax.rem(step, 2)

        @pl.when(step < 3)
        def _():
            for copy in left_copies(step + 1, 1 - slot):
                copy.start()
        for copy in left_copies(step, slot):
            copy.wait()

        for n in range(2 * width // tile):
            cols = pl.ds(n * tile, tile)
            acc[step, :, cols] = dot_tokens(left_buf[slot], right_buf[:, cols])
        for k in range(4):
            @pl.when(step == k)
            def _():
                hi_copy(k, (k + 1) % 4).start()
        for copy in lo_copies(step):
            copy.start()

    for step in range(4):
        hi_copy(step, (step + 1) % 4).wait()
        for copy in lo_copies(step):
            copy.wait()


def column_parts(lefts, rights, width, info, shared, split_right, n_chunks):
    n_tok = 4 * lefts[0].shape[0]
    any_spec = pl.BlockSpec(memory_space=pl.ANY)
    f32 = jnp.float32
    outs = [jax.ShapeDtypeStruct((512, width), f32)] * 4 + [jax.ShapeDtypeStruct((4, 128, width), f32)] * 4
    result = pl.pallas_call(
        functools.partial(column_kernel, shared, split_right, width, n_chunks),
        grid_spec=pltpu.PrefetchScalarGridSpec(
            num_scalar_prefetch=1,
            grid=(1,),
            in_specs=[any_spec] * (len(lefts) + len(rights)),
            out_specs=[any_spec] * 8,
            scratch_shapes=[
                pltpu.VMEM((2, n_tok, 512), jnp.bfloat16),
                pltpu.VMEM((n_tok, 2 * width), jnp.bfloat16),
                pltpu.VMEM((4, 512, 2 * width), f32),
                pltpu.SemaphoreType.DMA((2, 7)),
                pltpu.SemaphoreType.DMA((2, 7)),
                pltpu.SemaphoreType.DMA((4,)),
                pltpu.SemaphoreType.DMA((4, 4, 4)),
            ],
        ),
        out_shape=outs,
        compiler_params=pltpu.CompilerParams(vmem_limit_bytes=40 << 20),
        cost_estimate=pl.CostEstimate(flops=2 * n_tok * 2048 * 2 * width, bytes_accessed=30 << 20, transcendentals=0),
    )(info, *lefts, *rights)
    return result[:4], result[4:]


def row_kernel(shared, hi_mode, width, info, *refs):
    lefts, refs = refs[:4], refs[4:]
    n_right = 7 if shared else 4
    rights, refs = refs[:n_right], refs[n_right:]
    outs, refs = refs[:4], refs[4:]
    left_buf, right_buf, acc, left_sem, right_sem, out_sem = refs
    p_at, block, core = info[0], info[2], info[3]
    n_own = rights[0].shape[0]
    half = n_own // 2
    rows_each = width // 16
    plan = load_plan(n_own, shared)
    left_copies = []
    for k, (source, which, rows, first) in enumerate(plan):
        col = pl.multiple_of(block * width, 128) if source == 0 else 0
        left_copies.append(pltpu.make_async_copy(
            lefts[source].at[pl.ds(row_start(which, half, core), rows), pl.ds(col, width)],
            left_buf.at[pl.ds(first, rows), :], left_sem.at[k]))
    for copy in left_copies:
        copy.start()

    def right_copies(step, slot):
        col = pl.multiple_of(step * 512, 512)
        for k, (source, which, rows, first) in enumerate(plan):
            ref = rights[k] if shared else rights[source]
            yield pltpu.make_async_copy(
                ref.at[:, pl.ds(col, 512)], right_buf.at[slot, pl.ds(first, rows), :], right_sem.at[slot, k])

    for copy in right_copies(0, 0):
        copy.start()
    for copy in left_copies:
        copy.wait()

    def out_copies(step):
        cols = pl.ds(pl.multiple_of(step * 512, 512), 512)
        for d in range(4):
            slot = lax.rem(p_at + d, 4)
            if hi_mode:
                first = pl.multiple_of(slot * (4 * rows_each), 8)
                yield pltpu.make_async_copy(
                    acc.at[step, pl.ds(first, 4 * rows_each), :], outs[d].at[:, cols], out_sem.at[step, d, 0])
            else:
                for hi in range(4):
                    first = pl.multiple_of(hi * (4 * rows_each) + slot * rows_each, 8)
                    yield pltpu.make_async_copy(
                        acc.at[step, pl.ds(first, rows_each), :], outs[d].at[hi, :, cols], out_sem.at[step, d, hi])

    @pl.loop(0, 4)
    def _(step):
        slot = lax.rem(step, 2)

        @pl.when(step < 3)
        def _():
            for copy in right_copies(step + 1, 1 - slot):
                copy.start()
        for copy in right_copies(step, slot):
            copy.wait()
        acc[step] = dot_tokens(left_buf[...], right_buf[slot])
        for copy in out_copies(step):
            copy.start()

    for step in range(4):
        for copy in out_copies(step):
            copy.wait()


def row_parts(lefts, rights, width, info, shared, hi_mode):
    n_tok = 4 * rights[0].shape[0]
    any_spec = pl.BlockSpec(memory_space=pl.ANY)
    f32 = jnp.float32
    rows_each = width // 16
    shape = (4 * rows_each, 2048) if hi_mode else (4, rows_each, 2048)
    return pl.pallas_call(
        functools.partial(row_kernel, shared, hi_mode, width),
        grid_spec=pltpu.PrefetchScalarGridSpec(
            num_scalar_prefetch=1,
            grid=(1,),
            in_specs=[any_spec] * (len(lefts) + len(rights)),
            out_specs=[any_spec] * 4,
            scratch_shapes=[
                pltpu.VMEM((n_tok, width), jnp.bfloat16),
                pltpu.VMEM((2, n_tok, 512), jnp.bfloat16),
                pltpu.VMEM((4, width, 512), f32),
                pltpu.SemaphoreType.DMA((7,)),
                pltpu.SemaphoreType.DMA((2, 7)),
                pltpu.SemaphoreType.DMA((4, 4, 4)),
            ],
        ),
        out_shape=[jax.ShapeDtypeStruct(shape, f32)] * 4,
        compiler_params=pltpu.CompilerParams(vmem_limit_bytes=40 << 20),
        cost_estimate=pl.CostEstimate(flops=2 * n_tok * 2048 * width, bytes_accessed=20 << 20, transcendentals=0),
    )(info, *lefts, *rights)


def rms_scale(values, gain):
    mean_square = jnp.mean(values * values, axis=-1, keepdims=True)
    return values * lax.rsqrt(mean_square + NORM_EPS) * gain


def gate_mix(gate_pre, up_pre):
    return (jax.nn.silu(gate_pre.astype(jnp.float32)) * up_pre.astype(jnp.float32)).astype(jnp.bfloat16)


def build_mask(seg_query, seg_keys, query_pos, key_pos):
    causal = key_pos[None, :] <= query_pos[:, None]
    return causal[None] & (seg_keys[:, None, :] == seg_query[:, :, None])


def attend(query_heads, key_heads, value_heads, allowed):
    scores = jnp.einsum("bqkgd,bskd->bkgqs", query_heads, key_heads, preferred_element_type=jnp.float32) * (HEAD_DIM ** -0.5)
    scores = jnp.where(allowed[:, None, None], scores, -1e30)
    attn_probs = jax.nn.softmax(scores, axis=-1).astype(jnp.bfloat16)
    context = jnp.einsum("bkgqs,bskd->bqkgd", attn_probs, value_heads, preferred_element_type=jnp.float32)
    return context.astype(jnp.bfloat16)


def project(values, weight):
    return jnp.einsum("...d,df->...f", values, weight, preferred_element_type=jnp.float32)


def project_back(grads, weight):
    return jnp.einsum("...f,df->...d", grads, weight, preferred_element_type=jnp.float32)


def device_step(tokens, seg_ids, grad_out, gain_attn, gain_mlp, w_query, w_key, w_value, w_out, w_gate, w_up, w_down):
    n_rows, seq_len = tokens.shape[0], tokens.shape[1]
    n_tok = n_rows * seq_len
    width = tokens.shape[2]
    at = chip_coords()
    kv_heads = w_key.shape[1] // HEAD_DIM
    group_size = w_query.shape[1] // w_key.shape[1]
    flat = lambda v: v.reshape(n_tok, v.shape[-1])

    grad_all = gather_tokens(flat(grad_out), "z")
    x_float = tokens.astype(jnp.float32)
    norm_attn, attn_norm_vjp = jax.vjp(rms_scale, x_float, gain_attn)
    attn_in = norm_attn.astype(jnp.bfloat16)
    attn_in_all = gather_tokens(flat(attn_in), "y")
    query = project(attn_in, w_query).astype(jnp.bfloat16)
    key_proj = project(attn_in, w_key).astype(jnp.bfloat16)
    value_proj = project(attn_in, w_value).astype(jnp.bfloat16)
    positions = jnp.arange(seq_len)
    allowed = build_mask(seg_ids, seg_ids, positions, positions)
    context_heads, attn_vjp = jax.vjp(
        functools.partial(attend, allowed=allowed),
        query.reshape(n_rows, seq_len, kv_heads, group_size, HEAD_DIM),
        key_proj.reshape(n_rows, seq_len, kv_heads, HEAD_DIM),
        value_proj.reshape(n_rows, seq_len, kv_heads, HEAD_DIM),
    )
    context = context_heads.reshape(n_rows, seq_len, -1)
    attn_sum = sum_cores(project(context, w_out).astype(jnp.bfloat16))
    hidden_float = (x_float + attn_sum).astype(jnp.bfloat16).astype(jnp.float32)
    norm_mlp, mlp_norm_vjp = jax.vjp(rms_scale, hidden_float, gain_mlp)
    mlp_in = norm_mlp.astype(jnp.bfloat16)
    mlp_in_all = gather_tokens_shared(flat(mlp_in), "x")
    gate_pre = project(mlp_in, w_gate).astype(jnp.bfloat16)
    up_pre = project(mlp_in, w_up).astype(jnp.bfloat16)
    mixed_act, mix_vjp = jax.vjp(gate_mix, gate_pre, up_pre)
    mixed_all = [flat(mixed_act)] + exchange_columns(flat(mixed_act), "z", at)
    mlp_sum = sum_cores(project(mixed_act, w_down).astype(jnp.bfloat16))
    layer_out = (hidden_float + mlp_sum).astype(jnp.bfloat16)
    d_mixed = project_back(grad_out, w_down).astype(jnp.bfloat16)
    d_gate, d_up = mix_vjp(d_mixed)
    d_gate_all = [flat(d_gate)] + exchange_columns(flat(d_gate), "x", at)
    d_up_all = [flat(d_up)] + exchange_columns(flat(d_up), "x", at)
    d_mlp_in = sum_cores((project_back(d_gate, w_gate) + project_back(d_up, w_up)).astype(jnp.bfloat16))
    d_hidden_part, gain_mlp_part = mlp_norm_vjp(d_mlp_in)
    d_hidden = grad_out.astype(jnp.float32) + d_hidden_part
    d_hidden_b = d_hidden.astype(jnp.bfloat16)
    d_context = project_back(d_hidden_b, w_out).astype(jnp.bfloat16)
    d_query_h, d_key_h, d_value_h = attn_vjp(d_context.reshape(context_heads.shape))
    d_query = d_query_h.reshape(n_rows, seq_len, -1)
    d_key = d_key_h.reshape(n_rows, seq_len, -1)
    d_value = d_value_h.reshape(n_rows, seq_len, -1)
    d_attn_in = sum_cores((project_back(d_query, w_query) + project_back(d_key, w_key) + project_back(d_value, w_value)).astype(jnp.bfloat16))
    d_tokens_part, gain_attn_part = attn_norm_vjp(d_attn_in)
    grad_tokens = (d_hidden + d_tokens_part).astype(jnp.bfloat16)
    gains = jnp.stack([gain_attn_part, gain_mlp_part])

    core = lax.axis_index("tp")
    info = lambda p_at, lo_at, block: jnp.stack([at[p_at], at[lo_at], at[block], core]).astype(jnp.int32)
    down_parts = row_parts(mixed_all, grad_all, mixed_act.shape[-1] // 4, info("x", "x", "z"), False, False)
    g_down = scatter_parts(down_parts, "x")
    gate_parts, up_parts = column_parts(mlp_in_all, d_gate_all + d_up_all, d_gate.shape[-1] // 4, info("z", "y", "x"), True, False, 1)
    g_gate = scatter_parts(gate_parts, "z").reshape(4, 128, -1)
    g_up = scatter_parts(up_parts, "y")

    d_hidden_all = gather_tokens_shared(flat(d_hidden_b), "z")
    context_all = [flat(context)] + exchange_columns(flat(context), "z", at)
    out_parts = row_parts(context_all, d_hidden_all, context.shape[-1] // 4, info("x", "x", "z"), True, False)
    n_q = w_query.shape[1] // 4
    n_k = w_key.shape[1] // 4
    n_own = width // 64

    def qkv_block(b):
        return jnp.concatenate(
            [lax.dynamic_slice_in_dim(flat(v), (b % 4) * (v.shape[-1] // 4), v.shape[-1] // 4, 1) for v in (d_query, d_key, d_value)], axis=1)

    qkv_all = [qkv_block(at["y"])] + [shift(qkv_block(at["y"] + d), "y", d) for d in STEPS]
    q_parts, kv_parts = column_parts(attn_in_all, qkv_all, n_q, info("z", "x", "y"), False, True, 4)

    def turns(values, here, dim=0):
        return [pick(values, here + d, dim) for d in range(4)]

    gate_turn, up_turn, down_turn = turns(g_gate, at["y"]), turns(g_up, at["z"]), turns(g_down, at["y"])
    got = exchange([
        ("z", q_parts[1:]), ("x", kv_parts[1:]), ("x", out_parts[1:]), ("y", gate_turn[1:]), ("z", up_turn[1:]), ("y", down_turn[1:]),
        ("x", [gains] * 3),
    ], 1)
    g_q = add_parts([q_parts[0]] + got[0]).reshape(4, 4, n_own, n_q)
    g_kv = add_parts([kv_parts[0]] + got[1])
    g_out = add_parts([out_parts[0]] + got[2])
    pair = jnp.stack([add_parts([gate_turn[0]] + got[3]), add_parts([up_turn[0]] + got[4])]).reshape(2, 4, n_own, -1)
    grad_down = add_parts([down_turn[0]] + got[5])
    gains = add_parts(in_source_order(gains, got[6], at["x"]))
    q_turn, kv_turn, out_turn = turns(g_q, at["x"], 1), turns(g_kv, at["z"]), turns(g_out, at["y"])
    pair_turn = turns(pair, at["x"], 1)
    got = exchange([
        ("x", q_turn[1:]), ("z", kv_turn[1:]), ("y", out_turn[1:]), ("x", pair_turn[1:]), ("y", [gains] * 3),
    ], 2)
    g_qkv = jnp.concatenate([
        add_parts([q_turn[0]] + got[0]), add_parts([kv_turn[0]] + got[1]).reshape(4, n_own, -1)], axis=2)
    grad_out_w = add_parts([out_turn[0]] + got[2])
    ordered = in_source_order(pair_turn[0], got[3], at["x"])
    grad_gate = jnp.concatenate([o[0] for o in ordered], axis=1)
    grad_up = jnp.concatenate([o[1] for o in ordered], axis=1)
    gains = add_parts(in_source_order(gains, got[4], at["y"]))
    qkv_turn = turns(g_qkv, at["y"])
    got = exchange([("y", qkv_turn[1:]), ("z", [gains] * 3)], 3)
    ordered = in_source_order(qkv_turn[0], got[0], at["y"])
    gains = add_parts(in_source_order(gains, got[1], at["z"]))
    grad_query = jnp.concatenate([o[:, :n_q] for o in ordered], axis=1)
    grad_key = jnp.concatenate([o[:, n_q:n_q + n_k] for o in ordered], axis=1)
    grad_value = jnp.concatenate([o[:, n_q + n_k:] for o in ordered], axis=1)
    return (
        layer_out,
        grad_tokens,
        gains[0],
        gains[1],
        grad_query,
        grad_key,
        grad_value,
        grad_out_w,
        grad_gate,
        grad_up,
        grad_down,
    )


def solution(mesh):
    row_spec = P(("pod", "dp"), None, None)
    seg_spec = P(("pod", "dp"), None)
    col_spec = P(None, "tp")
    row_split = P("tp", None)
    grad_col = P(("pod", "dp"), "tp")
    grad_row = P(("pod", "tp", "dp"), None)
    gain_spec = P("pod")
    return jax.shard_map(
        device_step,
        mesh=mesh,
        in_specs=(row_spec, seg_spec, row_spec, P(), P(), col_spec, col_spec, col_spec, row_split, col_spec, col_spec, row_split),
        out_specs=(row_spec, row_spec, gain_spec, gain_spec, grad_col, grad_col, grad_col, grad_row, grad_col, grad_col, grad_row),
        check_vma=False,
    )
```

```python
import functools
import jax
import jax.numpy as jnp
from jax import lax
from jax.experimental import pallas as pl
from jax.experimental.pallas import tpu as pltpu
from jax.sharding import PartitionSpec as P


HEAD_DIM = 128
NORM_EPS = 1e-5
STEPS = (1, 3, 2)
STRIDE = {"z": 16, "y": 4, "x": 1}


def chip_coords():
    chip = lax.axis_index("dp")
    return {"z": chip // 16, "y": (chip // 4) % 4, "x": chip % 4}


def to_chip(chip, **coord):
    parts = {"z": chip // 16, "y": (chip // 4) % 4, "x": chip % 4}
    parts.update(coord)
    return 16 * (parts["z"] % 4) + 4 * (parts["y"] % 4) + parts["x"] % 4


def coord_of(chip, axis):
    return (chip // STRIDE[axis]) % 4


def shift(values, axis, step):
    pairs = [(c, to_chip(c, **{axis: coord_of(c, axis) + step})) for c in range(64)]
    return lax.ppermute(values, "dp", pairs)


def swap_cores(values):
    return lax.ppermute(values, "tp", [(0, 1), (1, 0)])


def sum_cores(part):
    other = swap_cores(part)
    return lax.reduce_precision(part.astype(jnp.float32) + other.astype(jnp.float32), 8, 7)


def pick(values, index, dim):
    return lax.dynamic_index_in_dim(values, index % values.shape[dim], dim, keepdims=False)


def gather_tokens(values, axis):
    return [values] + [shift(values, axis, d) for d in STEPS]


def send_row(values, axis):
    half = values.shape[0] // 2
    row = lax.dynamic_slice_in_dim(values, lax.axis_index("tp") * half, half, 0)
    return [shift(row, axis, d) for d in STEPS]


def share_rows(values, direct):
    return [values] + direct + [swap_cores(v) for v in direct]


def exchange_columns(values, axis, at):
    width = values.shape[1] // 4
    return [shift(lax.dynamic_slice_in_dim(values, ((at[axis] + d) % 4) * width, width, 1), axis, d) for d in STEPS]


def add_parts(parts):
    return parts[0] + parts[1] + parts[2] + parts[3]


def exchange_kernel(routes, *refs):
    n = len(routes)
    sources, targets, (send_sem, recv_sem) = refs[:n], refs[n:2 * n], refs[2 * n:]
    chip = lax.axis_index("dp")

    def chip_at(offset, sign):
        return to_chip(chip, **{a: coord_of(chip, a) + sign * offset[k] + 4 for k, a in enumerate("zyx")})

    barrier = pltpu.get_barrier_semaphore()
    offsets = sorted(set(routes))
    for offset in offsets:
        pl.semaphore_signal(barrier, inc=1, device_id={"dp": chip_at(offset, -1)}, device_id_type=pl.DeviceIdType.MESH)
    pl.semaphore_wait(barrier, len(offsets))
    copies = []
    for k, offset in enumerate(routes):
        copies.append(pltpu.make_async_remote_copy(
            src_ref=sources[k], dst_ref=targets[k], send_sem=send_sem.at[k], recv_sem=recv_sem.at[k],
            device_id={"dp": chip_at(offset, 1)}, device_id_type=pl.DeviceIdType.MESH))
    for copy in copies:
        copy.start()
    for copy in copies:
        copy.wait()


def along(axis):
    return [tuple(d if a == axis else 0 for a in "zyx") for d in (2, 1, 3)]


def exchange(groups, call_id):
    entries = [(g, offset, value) for g, group in enumerate(groups) for offset, value in group]
    values = [value for _, _, value in entries]
    any_spec = pl.BlockSpec(memory_space=pl.ANY)
    n = len(values)
    sent = sum(v.size * v.dtype.itemsize for v in values)
    out = pl.pallas_call(
        functools.partial(exchange_kernel, [offset for _, offset, _ in entries]),
        in_specs=[any_spec] * n,
        out_specs=[any_spec] * n,
        out_shape=[jax.ShapeDtypeStruct(v.shape, v.dtype) for v in values],
        scratch_shapes=[pltpu.SemaphoreType.DMA((n,)), pltpu.SemaphoreType.DMA((n,))],
        compiler_params=pltpu.CompilerParams(collective_id=call_id, has_side_effects=True),
        cost_estimate=pl.CostEstimate(flops=0, bytes_accessed=2 * sent, transcendentals=0),
    )(*values)
    out = lax.optimization_barrier(out)
    got = [{} for _ in groups]
    for (g, offset, _), value in zip(entries, out):
        got[g][offset] = value
    return got


def line_group(axis, turn):
    return [(offset, turn[sum(offset)]) for offset in along(axis)]


def line_values(got):
    by_distance = {sum(offset): value for offset, value in got.items()}
    return [by_distance[d] for d in (1, 2, 3)]


def in_source_order(own, received, here):
    stacked = jnp.stack([own] + received)
    return [pick(stacked, here - b, 0) for b in range(4)]


def load_plan(own_rows, shared):
    half = own_rows // 2
    if not shared:
        return [(k, "all", own_rows, own_rows * k) for k in range(4)]
    plan = [(0, "all", own_rows, 0)]
    for group, which in enumerate(("mine", "other")):
        for k in range(3):
            plan.append((k + 1, which, half, own_rows + half * (3 * group + k)))
    return plan


def row_start(which, half, core):
    if which == "all":
        return 0
    return pl.multiple_of((core if which == "mine" else 1 - core) * half, half)


def dot_tokens(left, right):
    return lax.dot_general(left, right, (((0,), (0,)), ((), ())), preferred_element_type=jnp.float32)


def column_kernel(hi_mode, width, n_chunks, info, *refs):
    lefts, rights, outs, refs = refs[:7], refs[7:11], refs[11:15], refs[15:]
    left_buf, right_buf, acc, left_sem, right_sem, out_sem = refs
    hi_at, lo_at, block, core = info[0], info[1], info[2], info[3]
    n_own = lefts[0].shape[0]
    half = n_own // 2
    plan = load_plan(n_own, True)

    right_copies = []
    for k, (source, which, rows, first) in enumerate(plan):
        whole = rights[source].shape[1] == width
        col = 0 if whole else pl.multiple_of(block * width, 128)
        right_copies.append(pltpu.make_async_copy(
            rights[source].at[pl.ds(row_start(which, half, core), rows), pl.ds(col, width)],
            right_buf.at[pl.ds(first, rows), :], right_sem.at[k]))
    for copy in right_copies:
        copy.start()

    def row_block(step):
        return lax.rem(hi_at + step + 1, 4)

    def left_copies(step, slot):
        col = pl.multiple_of(row_block(step) * 512, 512)
        for k, (source, which, rows, first) in enumerate(plan):
            yield pltpu.make_async_copy(
                lefts[k].at[:, pl.ds(col, 512)], left_buf.at[slot, pl.ds(first, rows), :], left_sem.at[slot, k])

    for copy in left_copies(0, 0):
        copy.start()
    for copy in right_copies:
        copy.wait()

    def lo_copies(step):
        rows = 128 // n_chunks
        for d in range(4):
            for k in range(n_chunks):
                first = pl.multiple_of(k * 128 + lax.rem(lo_at + d, 4) * rows, rows)
                yield pltpu.make_async_copy(
                    acc.at[step, pl.ds(first, rows), :], outs[d].at[row_block(step), pl.ds(k * rows, rows), :], out_sem.at[step, d, k])

    def hi_copy(step, d):
        return pltpu.make_async_copy(acc.at[step], outs[d], out_sem.at[step, 0, 0])

    tile = 512 if width % 512 == 0 else 256

    @pl.loop(0, 4)
    def _(step):
        slot = lax.rem(step, 2)

        @pl.when(step < 3)
        def _():
            for copy in left_copies(step + 1, 1 - slot):
                copy.start()

        for copy in left_copies(step, slot):
            copy.wait()

        for n in range(width // tile):
            cols = pl.ds(n * tile, tile)
            acc[step, :, cols] = dot_tokens(left_buf[slot], right_buf[:, cols])
        if hi_mode:
            for k in range(4):
                @pl.when(step == k)
                def _():
                    hi_copy(k, (k + 1) % 4).start()
        else:
            for copy in lo_copies(step):
                copy.start()

    for step in range(4):
        if hi_mode:
            hi_copy(step, (step + 1) % 4).wait()
        else:
            for copy in lo_copies(step):
                copy.wait()


def column_parts(lefts, rights, width, info, hi_mode, n_chunks):
    n_tok = 4 * lefts[0].shape[0]
    any_spec = pl.BlockSpec(memory_space=pl.ANY)
    f32 = jnp.float32
    return pl.pallas_call(
        functools.partial(column_kernel, hi_mode, width, n_chunks),
        grid_spec=pltpu.PrefetchScalarGridSpec(
            num_scalar_prefetch=1,
            grid=(1,),
            in_specs=[any_spec] * (len(lefts) + len(rights)),
            out_specs=[any_spec] * 4,
            scratch_shapes=[
                pltpu.VMEM((2, n_tok, 512), jnp.bfloat16),
                pltpu.VMEM((n_tok, width), jnp.bfloat16),
                pltpu.VMEM((4, 512, width), f32),
                pltpu.SemaphoreType.DMA((2, 7)),
                pltpu.SemaphoreType.DMA((7,)),
                pltpu.SemaphoreType.DMA((4, 4, 4)),
            ],
        ),
        out_shape=[jax.ShapeDtypeStruct((512, width) if hi_mode else (4, 128, width), f32)] * 4,
        compiler_params=pltpu.CompilerParams(vmem_limit_bytes=32 << 20),
        cost_estimate=pl.CostEstimate(flops=2 * n_tok * 2048 * width, bytes_accessed=20 << 20, transcendentals=0),
    )(info, *lefts, *rights)


def row_kernel(shared, hi_mode, width, info, *refs):
    lefts, refs = refs[:4], refs[4:]
    n_right = 7 if shared else 4
    rights, refs = refs[:n_right], refs[n_right:]
    outs, refs = refs[:4], refs[4:]
    left_buf, right_buf, acc, left_sem, right_sem, out_sem = refs
    p_at, block, core = info[0], info[2], info[3]
    n_own = rights[0].shape[0]
    half = n_own // 2
    rows_each = width // 16
    plan = load_plan(n_own, shared)
    left_copies = []
    for k, (source, which, rows, first) in enumerate(plan):
        col = pl.multiple_of(block * width, 128) if source == 0 else 0
        left_copies.append(pltpu.make_async_copy(
            lefts[source].at[pl.ds(row_start(which, half, core), rows), pl.ds(col, width)],
            left_buf.at[pl.ds(first, rows), :], left_sem.at[k]))
    for copy in left_copies:
        copy.start()

    def right_copies(step, slot):
        col = pl.multiple_of(step * 512, 512)
        for k, (source, which, rows, first) in enumerate(plan):
            ref = rights[k] if shared else rights[source]
            yield pltpu.make_async_copy(
                ref.at[:, pl.ds(col, 512)], right_buf.at[slot, pl.ds(first, rows), :], right_sem.at[slot, k])

    for copy in right_copies(0, 0):
        copy.start()
    for copy in left_copies:
        copy.wait()

    def out_copies(step):
        cols = pl.ds(pl.multiple_of(step * 512, 512), 512)
        for d in range(4):
            slot = lax.rem(p_at + d, 4)
            if hi_mode:
                first = pl.multiple_of(slot * (4 * rows_each), 8)
                yield pltpu.make_async_copy(
                    acc.at[step, pl.ds(first, 4 * rows_each), :], outs[d].at[:, cols], out_sem.at[step, d, 0])
            else:
                for hi in range(4):
                    first = pl.multiple_of(hi * (4 * rows_each) + slot * rows_each, 8)
                    yield pltpu.make_async_copy(
                        acc.at[step, pl.ds(first, rows_each), :], outs[d].at[hi, :, cols], out_sem.at[step, d, hi])

    @pl.loop(0, 4)
    def _(step):
        slot = lax.rem(step, 2)

        @pl.when(step < 3)
        def _():
            for copy in right_copies(step + 1, 1 - slot):
                copy.start()

        for copy in right_copies(step, slot):
            copy.wait()
        acc[step] = dot_tokens(left_buf[...], right_buf[slot])
        for copy in out_copies(step):
            copy.start()

    for step in range(4):
        for copy in out_copies(step):
            copy.wait()


def row_parts(lefts, rights, width, info, shared, hi_mode):
    n_tok = 4 * rights[0].shape[0]
    any_spec = pl.BlockSpec(memory_space=pl.ANY)
    f32 = jnp.float32
    rows_each = width // 16
    shape = (4 * rows_each, 2048) if hi_mode else (4, rows_each, 2048)
    return pl.pallas_call(
        functools.partial(row_kernel, shared, hi_mode, width),
        grid_spec=pltpu.PrefetchScalarGridSpec(
            num_scalar_prefetch=1,
            grid=(1,),
            in_specs=[any_spec] * (len(lefts) + len(rights)),
            out_specs=[any_spec] * 4,
            scratch_shapes=[
                pltpu.VMEM((n_tok, width), jnp.bfloat16),
                pltpu.VMEM((2, n_tok, 512), jnp.bfloat16),
                pltpu.VMEM((4, width, 512), f32),
                pltpu.SemaphoreType.DMA((7,)),
                pltpu.SemaphoreType.DMA((2, 7)),
                pltpu.SemaphoreType.DMA((4, 4, 4)),
            ],
        ),
        out_shape=[jax.ShapeDtypeStruct(shape, f32)] * 4,
        compiler_params=pltpu.CompilerParams(vmem_limit_bytes=40 << 20),
        cost_estimate=pl.CostEstimate(flops=2 * n_tok * 2048 * width, bytes_accessed=20 << 20, transcendentals=0),
    )(info, *lefts, *rights)


def rms_scale(values, gain):
    mean_square = jnp.mean(values * values, axis=-1, keepdims=True)
    return values * lax.rsqrt(mean_square + NORM_EPS) * gain


def gate_mix(gate_pre, up_pre):
    return (jax.nn.silu(gate_pre.astype(jnp.float32)) * up_pre.astype(jnp.float32)).astype(jnp.bfloat16)


def masked_probs(query, key_t, allowed):
    scores = lax.dot_general(query, key_t, (((1,), (1,)), ((), ())), preferred_element_type=jnp.float32) * (HEAD_DIM ** -0.5)
    scores = jnp.where(allowed, scores, -1e30)
    weights = jnp.exp(scores - jnp.max(scores, axis=-1, keepdims=True))
    return weights / jnp.sum(weights, axis=-1, keepdims=True)


def visible(seg_col, seg_row):
    n = seg_row.shape[1]
    query_pos = lax.broadcasted_iota(jnp.int32, (n, n), 0)
    key_pos = lax.broadcasted_iota(jnp.int32, (n, n), 1)
    return (key_pos <= query_pos) & (seg_col == seg_row)


def attend_kernel(seg_col_ref, seg_row_ref, query_ref, key_ref, value_ref, context_ref):
    allowed = visible(seg_col_ref[0], seg_row_ref[0])
    for g in range(query_ref.shape[1] // HEAD_DIM):
        head = pl.ds(g * HEAD_DIM, HEAD_DIM)
        probs = masked_probs(query_ref[:, head], key_ref[...], allowed).astype(jnp.bfloat16)
        context_ref[:, head] = jnp.dot(probs, value_ref[...], preferred_element_type=jnp.float32).astype(jnp.bfloat16)


def attend_back_kernel(seg_col_ref, seg_row_ref, query_ref, key_ref, value_ref, grad_ref, d_query_ref, d_key_ref, d_value_ref):
    allowed = visible(seg_col_ref[0], seg_row_ref[0])
    d_key = d_value = 0.0
    for g in range(query_ref.shape[1] // HEAD_DIM):
        head = pl.ds(g * HEAD_DIM, HEAD_DIM)
        query, grad = query_ref[:, head], grad_ref[:, head]
        probs = masked_probs(query, key_ref[...], allowed)
        d_value = d_value + dot_tokens(probs.astype(jnp.bfloat16), grad)
        d_probs = lax.dot_general(grad, value_ref[...], (((1,), (1,)), ((), ())), preferred_element_type=jnp.float32)
        d_probs = d_probs.astype(jnp.bfloat16).astype(jnp.float32)
        d_scores = probs * (d_probs - jnp.sum(d_probs * probs, axis=-1, keepdims=True))
        d_scores = (jnp.where(allowed, d_scores, 0.0) * (HEAD_DIM ** -0.5)).astype(jnp.bfloat16)
        d_query_ref[:, head] = jnp.dot(d_scores, key_ref[...], preferred_element_type=jnp.float32).astype(jnp.bfloat16)
        d_key = d_key + dot_tokens(d_scores, query)
    d_key_ref[...] = d_key.astype(jnp.bfloat16)
    d_value_ref[...] = d_value.astype(jnp.bfloat16)


def attention_call(body, seg_ids, arrays, outs, n_dots):
    n_rows, seq_len = seg_ids.shape
    kv_heads = arrays[1].shape[1] // HEAD_DIM
    block = lambda v: pl.BlockSpec((seq_len, v.shape[1] // kv_heads), lambda r, h: (r, h))
    return pl.pallas_call(
        body,
        grid=(n_rows, kv_heads),
        in_specs=[pl.BlockSpec((1, seq_len, 1), lambda r, h: (r, 0, 0)), pl.BlockSpec((1, 1, seq_len), lambda r, h: (r, 0, 0))]
        + [block(v) for v in arrays],
        out_specs=[block(v) for v in outs],
        out_shape=[jax.ShapeDtypeStruct(v.shape, jnp.bfloat16) for v in outs],
        cost_estimate=pl.CostEstimate(
            flops=2 * n_dots * n_rows * seq_len * seq_len * arrays[0].shape[1] * 4, bytes_accessed=8 << 20, transcendentals=0),
    )(seg_ids[:, :, None], seg_ids[:, None, :], *arrays)


def project(values, weight):
    return jnp.einsum("...d,df->...f", values, weight, preferred_element_type=jnp.float32)


def project_back(grads, weight):
    return jnp.einsum("...f,df->...d", grads, weight, preferred_element_type=jnp.float32)


def layer_step(tokens, seg_ids, grad_out, gain_attn, gain_mlp, w_query, w_key, w_value, w_out, w_gate, w_up, w_down):
    n_tok = tokens.shape[0] * tokens.shape[1]
    width = tokens.shape[2]
    at = chip_coords()
    flat = lambda v: v.reshape(n_tok, v.shape[-1])
    out_shape = tokens.shape
    grad_out = flat(grad_out)
    core = lax.axis_index("tp")
    info = lambda p_at, lo_at, block: jnp.stack([at[p_at], at[lo_at], at[block], core]).astype(jnp.int32)

    grad_all = gather_tokens(grad_out, "z")
    x_float = flat(tokens).astype(jnp.float32)
    norm_attn, attn_norm_vjp = jax.vjp(rms_scale, x_float, gain_attn)
    attn_in = norm_attn.astype(jnp.bfloat16)
    attn_in_sent = send_row(attn_in, "x")
    query = project(attn_in, w_query).astype(jnp.bfloat16)
    key_proj = project(attn_in, w_key).astype(jnp.bfloat16)
    value_proj = project(attn_in, w_value).astype(jnp.bfloat16)
    (context,) = attention_call(attend_kernel, seg_ids, (query, key_proj, value_proj), (query,), 2)
    attn_sum = sum_cores(project(context, w_out).astype(jnp.bfloat16))
    hidden_float = (x_float + attn_sum).astype(jnp.bfloat16).astype(jnp.float32)
    norm_mlp, mlp_norm_vjp = jax.vjp(rms_scale, hidden_float, gain_mlp)
    mlp_in = norm_mlp.astype(jnp.bfloat16)
    mlp_in_sent_x, mlp_in_sent_y = send_row(mlp_in, "x"), send_row(mlp_in, "y")
    attn_in_all = share_rows(attn_in, attn_in_sent)
    gate_pre = project(mlp_in, w_gate).astype(jnp.bfloat16)
    up_pre = project(mlp_in, w_up).astype(jnp.bfloat16)
    mixed_act, mix_vjp = jax.vjp(gate_mix, gate_pre, up_pre)
    d_mixed = project_back(grad_out, w_down).astype(jnp.bfloat16)
    d_gate, d_up = mix_vjp(d_mixed)
    d_gate_all = [d_gate] + exchange_columns(d_gate, "x", at)
    d_up_all = [d_up] + exchange_columns(d_up, "y", at)
    mixed_all = [mixed_act] + exchange_columns(mixed_act, "z", at)
    context_all = [context] + exchange_columns(context, "z", at)
    d_mlp_part = (project_back(d_gate, w_gate) + project_back(d_up, w_up)).astype(jnp.bfloat16)
    d_mlp_in = sum_cores(d_mlp_part)
    mlp_in_x, mlp_in_y = share_rows(mlp_in, mlp_in_sent_x), share_rows(mlp_in, mlp_in_sent_y)
    mlp_part = project(mixed_act, w_down).astype(jnp.bfloat16)
    mlp_sum = sum_cores(mlp_part)
    layer_out = (hidden_float + mlp_sum).astype(jnp.bfloat16).reshape(out_shape)
    d_hidden_part, gain_mlp_part = mlp_norm_vjp(d_mlp_in)
    d_hidden = grad_out.astype(jnp.float32) + d_hidden_part
    d_hidden_b = d_hidden.astype(jnp.bfloat16)
    d_hidden_sent = send_row(d_hidden_b, "z")
    d_context = project_back(d_hidden_b, w_out).astype(jnp.bfloat16)
    d_query, d_key, d_value = attention_call(
        attend_back_kernel, seg_ids, (query, key_proj, value_proj, d_context), (query, key_proj, value_proj), 5)
    n_q = w_query.shape[1] // 4
    n_k = w_key.shape[1] // 4
    n_own = width // 64

    def qkv_block(b):
        return jnp.concatenate(
            [lax.dynamic_slice_in_dim(v, (b % 4) * (v.shape[-1] // 4), v.shape[-1] // 4, 1) for v in (d_query, d_key, d_value)], axis=1)

    qkv_all = [qkv_block(at["x"])] + [shift(qkv_block(at["x"] + d), "x", d) for d in STEPS]
    d_hidden_all = share_rows(d_hidden_b, d_hidden_sent)
    d_attn_part = (project_back(d_query, w_query) + project_back(d_key, w_key) + project_back(d_value, w_value)).astype(jnp.bfloat16)
    d_attn_in = sum_cores(d_attn_part)
    d_tokens_part, gain_attn_part = attn_norm_vjp(d_attn_in)
    grad_tokens = (d_hidden + d_tokens_part).astype(jnp.bfloat16).reshape(out_shape)
    gains = jnp.stack([gain_attn_part, gain_mlp_part])

    down_parts = row_parts(mixed_all, grad_all, mixed_act.shape[-1] // 4, info("y", "y", "z"), False, True)
    down_sent = [shift(down_parts[d], "y", d) for d in STEPS]
    gate_parts = column_parts(mlp_in_x, d_gate_all, d_gate.shape[-1] // 4, info("z", "y", "x"), True, 1)
    gate_sent = [shift(gate_parts[d], "z", d) for d in STEPS]
    up_parts = column_parts(mlp_in_y, d_up_all, d_up.shape[-1] // 4, info("z", "x", "y"), False, 4)
    up_sent = [shift(up_parts[d], "x", d) for d in STEPS]
    out_parts = row_parts(context_all, d_hidden_all, context.shape[-1] // 4, info("x", "x", "z"), True, False)
    out_sent = [shift(out_parts[d], "x", d) for d in STEPS]
    qkv_parts = column_parts(attn_in_all, qkv_all, qkv_all[1].shape[1], info("z", "y", "x"), False, 1)
    qkv_sent = [shift(qkv_parts[d], "y", d) for d in STEPS]
    g_down = add_parts([down_parts[0]] + down_sent).reshape(4, -1, width)
    g_gate = add_parts([gate_parts[0]] + gate_sent).reshape(4, 128, -1)
    g_up = add_parts([up_parts[0]] + up_sent)
    g_out = add_parts([out_parts[0]] + out_sent)
    g_qkv = add_parts([qkv_parts[0]] + qkv_sent)

    def turns(values, here, dim=0):
        return [pick(values, here + d, dim) for d in range(4)]

    gate_turn, up_turn, down_turn = turns(g_gate, at["y"]), turns(g_up, at["z"]), turns(g_down, at["x"])
    qkv_turn, out_turn = turns(g_qkv, at["z"]), turns(g_out, at["y"])
    got = exchange([
        line_group("y", gate_turn), line_group("z", up_turn), line_group("x", down_turn), line_group("z", qkv_turn),
        line_group("y", out_turn), line_group("x", [gains] * 4),
    ], 1)
    got = [line_values(g) for g in got]
    grad_down = add_parts([down_turn[0]] + got[2])
    grad_out_w = add_parts([out_turn[0]] + got[4])
    gains = add_parts(in_source_order(gains, got[5], at["x"]))
    gate_turn = turns(add_parts([gate_turn[0]] + got[0]).reshape(4, n_own, -1), at["x"])
    up_turn = turns(add_parts([up_turn[0]] + got[1]).reshape(4, n_own, -1), at["y"])
    qkv_turn = turns(add_parts([qkv_turn[0]] + got[3]).reshape(4, n_own, -1), at["x"])
    plane = [(dz, dy, 0) for dz in range(4) for dy in range(4) if dz or dy]
    got = exchange([
        line_group("x", gate_turn), line_group("y", up_turn), line_group("x", qkv_turn), [(offset, gains) for offset in plane],
    ], 2)
    grad_gate = jnp.concatenate(in_source_order(gate_turn[0], line_values(got[0]), at["x"]), axis=1)
    grad_up = jnp.concatenate(in_source_order(up_turn[0], line_values(got[1]), at["y"]), axis=1)
    ordered = in_source_order(qkv_turn[0], line_values(got[2]), at["x"])
    in_plane = jnp.stack([got[3].get((dz, dy, 0), gains) for dz in range(4) for dy in range(4)]).reshape(4, 4, 2, width)
    in_plane = jnp.stack([pick(in_plane, at["z"] - z, 0) for z in range(4)])
    in_plane = jnp.stack([pick(in_plane, at["y"] - y, 1) for y in range(4)])
    gains = jnp.sum(in_plane, axis=(0, 1))
    grad_query = jnp.concatenate([o[:, :n_q] for o in ordered], axis=1)
    grad_key = jnp.concatenate([o[:, n_q:n_q + n_k] for o in ordered], axis=1)
    grad_value = jnp.concatenate([o[:, n_q + n_k:] for o in ordered], axis=1)
    return (
        layer_out,
        grad_tokens,
        gains[0],
        gains[1],
        grad_query,
        grad_key,
        grad_value,
        grad_out_w,
        grad_gate,
        grad_up,
        grad_down,
    )


def solution(mesh):
    row_spec = P(("pod", "dp"), None, None)
    seg_spec = P(("pod", "dp"), None)
    col_spec = P(None, "tp")
    row_split = P("tp", None)
    grad_col = P(("pod", "dp"), "tp")
    grad_row = P(("pod", "tp", "dp"), None)
    gain_spec = P("pod")
    return jax.shard_map(
        layer_step,
        mesh=mesh,
        in_specs=(row_spec, seg_spec, row_spec, P(), P(), col_spec, col_spec, col_spec, row_split, col_spec, col_spec, row_split),
        out_specs=(row_spec, row_spec, gain_spec, gain_spec, grad_col, grad_col, grad_col, grad_row, grad_col, grad_col, grad_row),
        check_vma=False,
    )
```

```python
import functools
import jax
import jax.numpy as jnp
from jax import lax
from jax.experimental import pallas as pl
from jax.experimental.pallas import tpu as pltpu
from jax.sharding import PartitionSpec as P


HEAD_DIM = 128
NORM_EPS = 1e-5
STEPS = (1, 3, 2)
STRIDE = {"z": 16, "y": 4, "x": 1}


def chip_coords():
    chip = lax.axis_index("dp")
    return {"z": chip // 16, "y": (chip // 4) % 4, "x": chip % 4}


def to_chip(chip, **coord):
    parts = {"z": chip // 16, "y": (chip // 4) % 4, "x": chip % 4}
    parts.update(coord)
    return 16 * (parts["z"] % 4) + 4 * (parts["y"] % 4) + parts["x"] % 4


def coord_of(chip, axis):
    return (chip // STRIDE[axis]) % 4


def shift(values, axis, step):
    pairs = [(c, to_chip(c, **{axis: coord_of(c, axis) + step})) for c in range(64)]
    return lax.ppermute(values, "dp", pairs)


def swap_cores(values):
    return lax.ppermute(values, "tp", [(0, 1), (1, 0)])


def sum_cores(part):
    other = swap_cores(part)
    return lax.reduce_precision(part.astype(jnp.float32) + other.astype(jnp.float32), 8, 7)


def pick(values, index, dim):
    return lax.dynamic_index_in_dim(values, index % values.shape[dim], dim, keepdims=False)


def gather_tokens(values, axis):
    return [values] + [shift(values, axis, d) for d in STEPS]


def send_row(values, axis):
    half = values.shape[0] // 2
    row = lax.dynamic_slice_in_dim(values, lax.axis_index("tp") * half, half, 0)
    return [shift(row, axis, d) for d in STEPS]


def share_rows(values, direct):
    return [values] + direct + [swap_cores(v) for v in direct]


def exchange_columns(values, axis, at):
    width = values.shape[1] // 4
    return [shift(lax.dynamic_slice_in_dim(values, ((at[axis] + d) % 4) * width, width, 1), axis, d) for d in STEPS]


def add_parts(parts):
    return parts[0] + parts[1] + parts[2] + parts[3]


def exchange_kernel(entries, n_in, n_out, *refs):
    sources, targets, (send_sem, recv_sem) = refs[:n_in], refs[n_in:n_in + n_out], refs[n_in + n_out:]
    chip = lax.axis_index("dp")

    def chip_at(offset, sign):
        return to_chip(chip, **{a: coord_of(chip, a) + sign * offset[k] + 4 for k, a in enumerate("zyx")})

    barrier = pltpu.get_barrier_semaphore()
    offsets = sorted({entry[0] for entry in entries if any(entry[0])})
    for offset in offsets:
        pl.semaphore_signal(barrier, inc=1, device_id={"dp": chip_at(offset, -1)}, device_id_type=pl.DeviceIdType.MESH)
    pl.semaphore_wait(barrier, len(offsets))
    here = {a: coord_of(chip, a) for a in "zyx"}
    copies = []
    for k, (offset, source, view, target, place) in enumerate(entries):
        peer = chip_at(offset, 1)
        there = {a: coord_of(peer, a) for a in "zyx"}
        src, dst = view(sources[source], there), place(targets[target], here)
        if any(offset):
            copies.append(pltpu.make_async_remote_copy(
                src_ref=src, dst_ref=dst, send_sem=send_sem.at[k], recv_sem=recv_sem.at[k],
                device_id={"dp": peer}, device_id_type=pl.DeviceIdType.MESH))
        else:
            copies.append(pltpu.make_async_copy(src, dst, send_sem.at[k]))
    for copy in copies:
        copy.start()
    for copy in copies:
        copy.wait()


def along(axis):
    return [tuple(d if a == axis else 0 for a in "zyx") for d in (2, 1, 3)]


HERE = (0, 0, 0)


class Exchange:
    def __init__(self):
        self.values, self.shapes, self.entries = [], [], []

    def add(self, value, shape, offsets, view, place):
        self.values.append(value)
        self.shapes.append(shape)
        for offset in offsets:
            self.entries.append((offset, len(self.values) - 1, view, len(self.shapes) - 1, place(offset)))
        return len(self.shapes) - 1

    def line_sum(self, value, axis):
        return self.add(value, (3,) + value.shape[1:], along(axis), lambda ref, there: ref.at[there[axis]],
                        lambda offset: lambda ref, here: ref.at[sum(offset) - 1])

    def line_parts(self, parts, axis):
        for offset in along(axis):
            self.add(parts[sum(offset)], parts[0].shape, [offset], lambda ref, there: ref, lambda offset: lambda ref, here: ref)

    def line_columns(self, value, axis, first, width):
        return self.add(value, (value.shape[1], 4 * width), along(axis) + [HERE],
                        lambda ref, there: ref.at[there[axis], :, pl.ds(first, width)],
                        lambda offset: lambda ref, here: ref.at[:, pl.ds(pl.multiple_of(here[axis] * width, 128), width)])

    def to_all(self, value, offsets, slots, slot_of):
        return self.add(value, (slots,) + value.shape, offsets + [HERE], lambda ref, there: ref,
                        lambda offset: lambda ref, here: ref.at[slot_of(here)])

    def run(self, call_id):
        any_spec = pl.BlockSpec(memory_space=pl.ANY)
        n = len(self.entries)
        sent = sum(v.size * v.dtype.itemsize for v in self.values)
        out = pl.pallas_call(
            functools.partial(exchange_kernel, self.entries, len(self.values), len(self.shapes)),
            in_specs=[any_spec] * len(self.values),
            out_specs=[any_spec] * len(self.shapes),
            out_shape=[jax.ShapeDtypeStruct(shape, jnp.float32) for shape in self.shapes],
            scratch_shapes=[pltpu.SemaphoreType.DMA((n,)), pltpu.SemaphoreType.DMA((n,))],
            compiler_params=pltpu.CompilerParams(collective_id=call_id, has_side_effects=True),
            cost_estimate=pl.CostEstimate(flops=0, bytes_accessed=2 * sent, transcendentals=0),
        )(*self.values)
        return lax.optimization_barrier(out)


def load_plan(own_rows, shared):
    half = own_rows // 2
    if not shared:
        return [(k, "all", own_rows, own_rows * k) for k in range(4)]
    plan = [(0, "all", own_rows, 0)]
    for group, which in enumerate(("mine", "other")):
        for k in range(3):
            plan.append((k + 1, which, half, own_rows + half * (3 * group + k)))
    return plan


def row_start(which, half, core):
    if which == "all":
        return 0
    return pl.multiple_of((core if which == "mine" else 1 - core) * half, half)


def dot_tokens(left, right):
    return lax.dot_general(left, right, (((0,), (0,)), ((), ())), preferred_element_type=jnp.float32)


def column_kernel(hi_mode, width, n_chunks, info, *refs):
    lefts, rights, outs, refs = refs[:7], refs[7:11], refs[11:15], refs[15:]
    left_buf, right_buf, acc, left_sem, right_sem, out_sem = refs
    hi_at, lo_at, block, core = info[0], info[1], info[2], info[3]
    n_own = lefts[0].shape[0]
    half = n_own // 2
    plan = load_plan(n_own, True)

    right_copies = []
    for k, (source, which, rows, first) in enumerate(plan):
        whole = rights[source].shape[1] == width
        col = 0 if whole else pl.multiple_of(block * width, 128)
        right_copies.append(pltpu.make_async_copy(
            rights[source].at[pl.ds(row_start(which, half, core), rows), pl.ds(col, width)],
            right_buf.at[pl.ds(first, rows), :], right_sem.at[k]))
    for copy in right_copies:
        copy.start()

    def row_block(step):
        return lax.rem(hi_at + step + 1, 4)

    def left_copies(step, slot):
        col = pl.multiple_of(row_block(step) * 512, 512)
        for k, (source, which, rows, first) in enumerate(plan):
            yield pltpu.make_async_copy(
                lefts[k].at[:, pl.ds(col, 512)], left_buf.at[slot, pl.ds(first, rows), :], left_sem.at[slot, k])

    for copy in left_copies(0, 0):
        copy.start()
    for copy in right_copies:
        copy.wait()

    def lo_copies(step):
        rows = 128 // n_chunks
        for d in range(4):
            for k in range(n_chunks):
                first = pl.multiple_of(k * 128 + lax.rem(lo_at + d, 4) * rows, rows)
                yield pltpu.make_async_copy(
                    acc.at[step, pl.ds(first, rows), :], outs[d].at[row_block(step), pl.ds(k * rows, rows), :], out_sem.at[step, d, k])

    def hi_copy(step, d):
        return pltpu.make_async_copy(acc.at[step], outs[d], out_sem.at[step, 0, 0])

    tile = 512 if width % 512 == 0 else 256

    @pl.loop(0, 4)
    def _(step):
        slot = lax.rem(step, 2)

        @pl.when(step < 3)
        def _():
            for copy in left_copies(step + 1, 1 - slot):
                copy.start()

        for copy in left_copies(step, slot):
            copy.wait()

        for n in range(width // tile):
            cols = pl.ds(n * tile, tile)
            acc[step, :, cols] = dot_tokens(left_buf[slot], right_buf[:, cols])
        if hi_mode:
            for k in range(4):
                @pl.when(step == k)
                def _():
                    hi_copy(k, (k + 1) % 4).start()
        else:
            for copy in lo_copies(step):
                copy.start()

    for step in range(4):
        if hi_mode:
            hi_copy(step, (step + 1) % 4).wait()
        else:
            for copy in lo_copies(step):
                copy.wait()


def column_parts(lefts, rights, width, info, hi_mode, n_chunks):
    n_tok = 4 * lefts[0].shape[0]
    any_spec = pl.BlockSpec(memory_space=pl.ANY)
    f32 = jnp.float32
    return pl.pallas_call(
        functools.partial(column_kernel, hi_mode, width, n_chunks),
        grid_spec=pltpu.PrefetchScalarGridSpec(
            num_scalar_prefetch=1,
            grid=(1,),
            in_specs=[any_spec] * (len(lefts) + len(rights)),
            out_specs=[any_spec] * 4,
            scratch_shapes=[
                pltpu.VMEM((2, n_tok, 512), jnp.bfloat16),
                pltpu.VMEM((n_tok, width), jnp.bfloat16),
                pltpu.VMEM((4, 512, width), f32),
                pltpu.SemaphoreType.DMA((2, 7)),
                pltpu.SemaphoreType.DMA((7,)),
                pltpu.SemaphoreType.DMA((4, 4, 4)),
            ],
        ),
        out_shape=[jax.ShapeDtypeStruct((512, width) if hi_mode else (4, 128, width), f32)] * 4,
        compiler_params=pltpu.CompilerParams(vmem_limit_bytes=32 << 20),
        cost_estimate=pl.CostEstimate(flops=2 * n_tok * 2048 * width, bytes_accessed=20 << 20, transcendentals=0),
    )(info, *lefts, *rights)


def row_kernel(shared, hi_mode, width, info, *refs):
    lefts, refs = refs[:4], refs[4:]
    n_right = 7 if shared else 4
    rights, refs = refs[:n_right], refs[n_right:]
    outs, refs = refs[:4], refs[4:]
    left_buf, right_buf, acc, left_sem, right_sem, out_sem = refs
    p_at, block, core = info[0], info[2], info[3]
    n_own = rights[0].shape[0]
    half = n_own // 2
    rows_each = width // 16
    plan = load_plan(n_own, shared)
    left_copies = []
    for k, (source, which, rows, first) in enumerate(plan):
        col = pl.multiple_of(block * width, 128) if source == 0 else 0
        left_copies.append(pltpu.make_async_copy(
            lefts[source].at[pl.ds(row_start(which, half, core), rows), pl.ds(col, width)],
            left_buf.at[pl.ds(first, rows), :], left_sem.at[k]))
    for copy in left_copies:
        copy.start()

    def right_copies(step, slot):
        col = pl.multiple_of(step * 512, 512)
        for k, (source, which, rows, first) in enumerate(plan):
            ref = rights[k] if shared else rights[source]
            yield pltpu.make_async_copy(
                ref.at[:, pl.ds(col, 512)], right_buf.at[slot, pl.ds(first, rows), :], right_sem.at[slot, k])

    for copy in right_copies(0, 0):
        copy.start()
    for copy in left_copies:
        copy.wait()

    def out_copies(step):
        cols = pl.ds(pl.multiple_of(step * 512, 512), 512)
        for d in range(4):
            slot = lax.rem(p_at + d, 4)
            if hi_mode:
                first = pl.multiple_of(slot * (4 * rows_each), 8)
                yield pltpu.make_async_copy(
                    acc.at[step, pl.ds(first, 4 * rows_each), :], outs[d].at[:, cols], out_sem.at[step, d, 0])
            else:
                for hi in range(4):
                    first = pl.multiple_of(hi * (4 * rows_each) + slot * rows_each, 8)
                    yield pltpu.make_async_copy(
                        acc.at[step, pl.ds(first, rows_each), :], outs[d].at[hi, :, cols], out_sem.at[step, d, hi])

    @pl.loop(0, 4)
    def _(step):
        slot = lax.rem(step, 2)

        @pl.when(step < 3)
        def _():
            for copy in right_copies(step + 1, 1 - slot):
                copy.start()

        for copy in right_copies(step, slot):
            copy.wait()
        acc[step] = dot_tokens(left_buf[...], right_buf[slot])
        for copy in out_copies(step):
            copy.start()

    for step in range(4):
        for copy in out_copies(step):
            copy.wait()


def row_parts(lefts, rights, width, info, shared, hi_mode):
    n_tok = 4 * rights[0].shape[0]
    any_spec = pl.BlockSpec(memory_space=pl.ANY)
    f32 = jnp.float32
    rows_each = width // 16
    shape = (4 * rows_each, 2048) if hi_mode else (4, rows_each, 2048)
    return pl.pallas_call(
        functools.partial(row_kernel, shared, hi_mode, width),
        grid_spec=pltpu.PrefetchScalarGridSpec(
            num_scalar_prefetch=1,
            grid=(1,),
            in_specs=[any_spec] * (len(lefts) + len(rights)),
            out_specs=[any_spec] * 4,
            scratch_shapes=[
                pltpu.VMEM((n_tok, width), jnp.bfloat16),
                pltpu.VMEM((2, n_tok, 512), jnp.bfloat16),
                pltpu.VMEM((4, width, 512), f32),
                pltpu.SemaphoreType.DMA((7,)),
                pltpu.SemaphoreType.DMA((2, 7)),
                pltpu.SemaphoreType.DMA((4, 4, 4)),
            ],
        ),
        out_shape=[jax.ShapeDtypeStruct(shape, f32)] * 4,
        compiler_params=pltpu.CompilerParams(vmem_limit_bytes=40 << 20),
        cost_estimate=pl.CostEstimate(flops=2 * n_tok * 2048 * width, bytes_accessed=20 << 20, transcendentals=0),
    )(info, *lefts, *rights)


def rms_scale(values, gain):
    mean_square = jnp.mean(values * values, axis=-1, keepdims=True)
    return values * lax.rsqrt(mean_square + NORM_EPS) * gain


def gate_mix(gate_pre, up_pre):
    return (jax.nn.silu(gate_pre.astype(jnp.float32)) * up_pre.astype(jnp.float32)).astype(jnp.bfloat16)


def masked_probs(query, key_t, allowed):
    scores = lax.dot_general(query, key_t, (((1,), (1,)), ((), ())), preferred_element_type=jnp.float32) * (HEAD_DIM ** -0.5)
    scores = jnp.where(allowed, scores, -1e30)
    weights = jnp.exp(scores - jnp.max(scores, axis=-1, keepdims=True))
    return weights / jnp.sum(weights, axis=-1, keepdims=True)


def visible(seg_col, seg_row):
    n = seg_row.shape[1]
    query_pos = lax.broadcasted_iota(jnp.int32, (n, n), 0)
    key_pos = lax.broadcasted_iota(jnp.int32, (n, n), 1)
    return (key_pos <= query_pos) & (seg_col == seg_row)


def attend_kernel(seg_col_ref, seg_row_ref, query_ref, key_ref, value_ref, context_ref):
    allowed = visible(seg_col_ref[0], seg_row_ref[0])
    for g in range(query_ref.shape[1] // HEAD_DIM):
        head = pl.ds(g * HEAD_DIM, HEAD_DIM)
        probs = masked_probs(query_ref[:, head], key_ref[...], allowed).astype(jnp.bfloat16)
        context_ref[:, head] = jnp.dot(probs, value_ref[...], preferred_element_type=jnp.float32).astype(jnp.bfloat16)


def attend_back_kernel(seg_col_ref, seg_row_ref, query_ref, key_ref, value_ref, grad_ref, d_query_ref, d_key_ref, d_value_ref):
    allowed = visible(seg_col_ref[0], seg_row_ref[0])
    d_key = d_value = 0.0
    for g in range(query_ref.shape[1] // HEAD_DIM):
        head = pl.ds(g * HEAD_DIM, HEAD_DIM)
        query, grad = query_ref[:, head], grad_ref[:, head]
        probs = masked_probs(query, key_ref[...], allowed)
        d_value = d_value + dot_tokens(probs.astype(jnp.bfloat16), grad)
        d_probs = lax.dot_general(grad, value_ref[...], (((1,), (1,)), ((), ())), preferred_element_type=jnp.float32)
        d_probs = d_probs.astype(jnp.bfloat16).astype(jnp.float32)
        d_scores = probs * (d_probs - jnp.sum(d_probs * probs, axis=-1, keepdims=True))
        d_scores = (jnp.where(allowed, d_scores, 0.0) * (HEAD_DIM ** -0.5)).astype(jnp.bfloat16)
        d_query_ref[:, head] = jnp.dot(d_scores, key_ref[...], preferred_element_type=jnp.float32).astype(jnp.bfloat16)
        d_key = d_key + dot_tokens(d_scores, query)
    d_key_ref[...] = d_key.astype(jnp.bfloat16)
    d_value_ref[...] = d_value.astype(jnp.bfloat16)


def attention_call(body, seg_ids, arrays, outs, n_dots):
    n_rows, seq_len = seg_ids.shape
    kv_heads = arrays[1].shape[1] // HEAD_DIM
    block = lambda v: pl.BlockSpec((seq_len, v.shape[1] // kv_heads), lambda r, h: (r, h))
    return pl.pallas_call(
        body,
        grid=(n_rows, kv_heads),
        in_specs=[pl.BlockSpec((1, seq_len, 1), lambda r, h: (r, 0, 0)), pl.BlockSpec((1, 1, seq_len), lambda r, h: (r, 0, 0))]
        + [block(v) for v in arrays],
        out_specs=[block(v) for v in outs],
        out_shape=[jax.ShapeDtypeStruct(v.shape, jnp.bfloat16) for v in outs],
        cost_estimate=pl.CostEstimate(
            flops=2 * n_dots * n_rows * seq_len * seq_len * arrays[0].shape[1] * 4, bytes_accessed=8 << 20, transcendentals=0),
    )(seg_ids[:, :, None], seg_ids[:, None, :], *arrays)


def project(values, weight):
    return jnp.einsum("...d,df->...f", values, weight, preferred_element_type=jnp.float32)


def project_back(grads, weight):
    return jnp.einsum("...f,df->...d", grads, weight, preferred_element_type=jnp.float32)


def layer_step(tokens, seg_ids, grad_out, gain_attn, gain_mlp, w_query, w_key, w_value, w_out, w_gate, w_up, w_down):
    n_tok = tokens.shape[0] * tokens.shape[1]
    width = tokens.shape[2]
    at = chip_coords()
    flat = lambda v: v.reshape(n_tok, v.shape[-1])
    out_shape = tokens.shape
    grad_out = flat(grad_out)
    core = lax.axis_index("tp")
    info = lambda p_at, lo_at, block: jnp.stack([at[p_at], at[lo_at], at[block], core]).astype(jnp.int32)

    grad_all = gather_tokens(grad_out, "z")
    x_float = flat(tokens).astype(jnp.float32)
    norm_attn, attn_norm_vjp = jax.vjp(rms_scale, x_float, gain_attn)
    attn_in = norm_attn.astype(jnp.bfloat16)
    attn_in_sent = send_row(attn_in, "x")
    query = project(attn_in, w_query).astype(jnp.bfloat16)
    key_proj = project(attn_in, w_key).astype(jnp.bfloat16)
    value_proj = project(attn_in, w_value).astype(jnp.bfloat16)
    (context,) = attention_call(attend_kernel, seg_ids, (query, key_proj, value_proj), (query,), 2)
    attn_sum = sum_cores(project(context, w_out).astype(jnp.bfloat16))
    hidden_float = (x_float + attn_sum).astype(jnp.bfloat16).astype(jnp.float32)
    norm_mlp, mlp_norm_vjp = jax.vjp(rms_scale, hidden_float, gain_mlp)
    mlp_in = norm_mlp.astype(jnp.bfloat16)
    mlp_in_sent_x, mlp_in_sent_y = send_row(mlp_in, "x"), send_row(mlp_in, "y")
    attn_in_all = share_rows(attn_in, attn_in_sent)
    gate_pre = project(mlp_in, w_gate).astype(jnp.bfloat16)
    up_pre = project(mlp_in, w_up).astype(jnp.bfloat16)
    mixed_act, mix_vjp = jax.vjp(gate_mix, gate_pre, up_pre)
    d_mixed = project_back(grad_out, w_down).astype(jnp.bfloat16)
    d_gate, d_up = mix_vjp(d_mixed)
    d_gate_all = [d_gate] + exchange_columns(d_gate, "x", at)
    d_up_all = [d_up] + exchange_columns(d_up, "y", at)
    mixed_all = [mixed_act] + exchange_columns(mixed_act, "z", at)
    context_all = [context] + exchange_columns(context, "z", at)
    d_mlp_part = (project_back(d_gate, w_gate) + project_back(d_up, w_up)).astype(jnp.bfloat16)
    d_mlp_in = sum_cores(d_mlp_part)
    mlp_in_x, mlp_in_y = share_rows(mlp_in, mlp_in_sent_x), share_rows(mlp_in, mlp_in_sent_y)
    mlp_part = project(mixed_act, w_down).astype(jnp.bfloat16)
    mlp_sum = sum_cores(mlp_part)
    layer_out = (hidden_float + mlp_sum).astype(jnp.bfloat16).reshape(out_shape)
    d_hidden_part, gain_mlp_part = mlp_norm_vjp(d_mlp_in)
    d_hidden = grad_out.astype(jnp.float32) + d_hidden_part
    d_hidden_b = d_hidden.astype(jnp.bfloat16)
    d_hidden_sent = send_row(d_hidden_b, "z")
    d_context = project_back(d_hidden_b, w_out).astype(jnp.bfloat16)
    d_query, d_key, d_value = attention_call(
        attend_back_kernel, seg_ids, (query, key_proj, value_proj, d_context), (query, key_proj, value_proj), 5)
    n_q = w_query.shape[1] // 4
    n_k = w_key.shape[1] // 4
    n_own = width // 64

    def qkv_block(b):
        return jnp.concatenate(
            [lax.dynamic_slice_in_dim(v, (b % 4) * (v.shape[-1] // 4), v.shape[-1] // 4, 1) for v in (d_query, d_key, d_value)], axis=1)

    qkv_all = [qkv_block(at["x"])] + [shift(qkv_block(at["x"] + d), "x", d) for d in STEPS]
    d_hidden_all = share_rows(d_hidden_b, d_hidden_sent)
    d_attn_part = (project_back(d_query, w_query) + project_back(d_key, w_key) + project_back(d_value, w_value)).astype(jnp.bfloat16)
    d_attn_in = sum_cores(d_attn_part)
    d_tokens_part, gain_attn_part = attn_norm_vjp(d_attn_in)
    grad_tokens = (d_hidden + d_tokens_part).astype(jnp.bfloat16).reshape(out_shape)
    gains = jnp.stack([gain_attn_part, gain_mlp_part])

    down_parts = row_parts(mixed_all, grad_all, mixed_act.shape[-1] // 4, info("y", "y", "z"), False, True)
    down_sent = [shift(down_parts[d], "y", d) for d in STEPS]
    gate_parts = column_parts(mlp_in_x, d_gate_all, d_gate.shape[-1] // 4, info("z", "y", "x"), True, 1)
    gate_sent = [shift(gate_parts[d], "z", d) for d in STEPS]
    up_parts = column_parts(mlp_in_y, d_up_all, d_up.shape[-1] // 4, info("z", "x", "y"), False, 4)
    up_sent = [shift(up_parts[d], "x", d) for d in STEPS]
    out_parts = row_parts(context_all, d_hidden_all, context.shape[-1] // 4, info("x", "x", "z"), True, False)
    qkv_parts = column_parts(attn_in_all, qkv_all, qkv_all[1].shape[1], info("z", "y", "x"), False, 1)
    qkv_sent = [shift(qkv_parts[d], "y", d) for d in STEPS]
    g_down = add_parts([down_parts[0]] + down_sent).reshape(4, -1, width)
    g_gate = add_parts([gate_parts[0]] + gate_sent).reshape(4, 128, -1)
    g_up = add_parts([up_parts[0]] + up_sent)
    g_qkv = add_parts([qkv_parts[0]] + qkv_sent)

    def line_total(value, here, got):
        return pick(value, here, 0) + got[0] + got[1] + got[2]

    first = Exchange()
    first.line_sum(g_gate, "y"), first.line_sum(g_up, "z"), first.line_parts(out_parts, "x")
    got = first.run(1)
    g_gate = line_total(g_gate, at["y"], got[0]).reshape(4, n_own, -1)
    g_up = line_total(g_up, at["z"], got[1]).reshape(4, n_own, -1)
    g_out = add_parts([out_parts[0]] + list(got[2:5]))
    second = Exchange()
    second.line_sum(g_qkv, "z"), second.line_sum(g_out, "y")
    second.line_columns(g_gate, "x", 0, g_gate.shape[2]), second.line_columns(g_up, "y", 0, g_up.shape[2])
    second.to_all(gains, along("x"), 4, lambda here: here["x"])
    second.line_sum(g_down, "x")
    got = second.run(2)
    g_qkv = line_total(g_qkv, at["z"], got[0]).reshape(4, n_own, -1)
    grad_out_w = line_total(g_out, at["y"], got[1])
    grad_gate, grad_up = got[2], got[3]
    gains = jnp.sum(got[4], axis=0)
    grad_down = line_total(g_down, at["x"], got[5])
    third = Exchange()
    third.line_columns(g_qkv, "x", 0, n_q), third.line_columns(g_qkv, "x", n_q, n_k), third.line_columns(g_qkv, "x", n_q + n_k, n_k)
    plane = [(dz, dy, 0) for dz in range(4) for dy in range(4) if dz or dy]
    third.to_all(gains, plane, 16, lambda here: 4 * here["z"] + here["y"])
    got = third.run(3)
    grad_query, grad_key, grad_value = got[:3]
    gains = jnp.sum(got[3], axis=0)
    return (
        layer_out,
        grad_tokens,
        gains[0],
        gains[1],
        grad_query,
        grad_key,
        grad_value,
        grad_out_w,
        grad_gate,
        grad_up,
        grad_down,
    )


def solution(mesh):
    row_spec = P(("pod", "dp"), None, None)
    seg_spec = P(("pod", "dp"), None)
    col_spec = P(None, "tp")
    row_split = P("tp", None)
    grad_col = P(("pod", "dp"), "tp")
    grad_row = P(("pod", "tp", "dp"), None)
    gain_spec = P("pod")
    return jax.shard_map(
        layer_step,
        mesh=mesh,
        in_specs=(row_spec, seg_spec, row_spec, P(), P(), col_spec, col_spec, col_spec, row_split, col_spec, col_spec, row_split),
        out_specs=(row_spec, row_spec, gain_spec, gain_spec, grad_col, grad_col, grad_col, grad_row, grad_col, grad_col, grad_row),
        check_vma=False,
    )
```
